256 devices in a mesh: expert: 64 (over x, z, core), pair: 2 (over y_lo), dp: 2 (over y_hi).
Axes of the slice: x: 4, y: 4 (y_hi: 2, y_lo: 2; y = y_hi * 2 + y_lo), z: 8, core: 2. Of those that a mesh axis runs over, the one named last changes fastest.
Arguments:
- tokens: bfloat16 [1024, 196, 768], P(('expert', 'pair', 'dp')), may hold values from -96 to 96
- phi: bfloat16 [768, 128], replicated, may hold values from -0.25 to 0.25
- w_in: bfloat16 [64, 768, 3072], P('expert', None, 'pair'), may hold values from -0.21875 to 0.21875
- w_out: bfloat16 [64, 3072, 768], P('expert', 'pair'), may hold values from -0.109375 to 0.109375
- slot_out: bfloat16 [1024, 128, 768], P(('expert', 'pair', 'dp')), may hold values from -6 to 6
- grad_out: bfloat16 [1024, 196, 768], P(('expert', 'pair', 'dp')), may hold values from -6 to 6
Outputs:
- token_grad: bfloat16 [1024, 196, 768], P(('expert', 'pair', 'dp'))
- phi_grad: float32 [768, 128], replicated
- grad_w_in: bfloat16 [64, 768, 3072], P('expert', 'dp', 'pair')
- grad_w_out: bfloat16 [64, 3072, 768], P('expert', 'pair', 'dp')
The draws below stay inside these ranges and needn't reach their ends.
All inputs are finite; a program needn't handle non-finite values.
Results may differ from the reference program's by a relative error of at most 0.0086.
Values may be sent and summed in bfloat16 or wider, within the bound.
No kernel may reach another device: no remote copies, remote signals or barrier semaphores. Data moves between devices by JAX's collectives and lax.ppermute only.
A program may use at most 128 MiB of HBM per device.

```python
import jax
import jax.numpy as jnp
from jax import lax

D = 768
FF = 3072
TOKENS_IMG = 196
SLOTS = 2
IMG_DEV = 4
EXPERTS = 64
IMAGES = 1024
N_DP = 2


def phi_table(key):
    raw = jax.random.normal(jax.random.fold_in(key, 101), (D, EXPERTS * SLOTS), jnp.float32)
    scaled = jnp.clip(raw, -6.0, 6.0) * D ** (-0.5)
    return jnp.clip(scaled, -0.25, 0.25)


def draw_phi(key, part):
    return phi_table(key).astype(jnp.bfloat16)


def draw_tokens(key, part):
    drawn = jax.random.normal(jax.random.fold_in(key, 202), (IMAGES, TOKENS_IMG, D), jnp.float32)
    return jnp.clip(drawn, -6.0, 6.0).astype(jnp.bfloat16)


def block_levels(own_key, extent, shards, low, top_value):
    gain = 1.0
    for axis_at, blocks in shards:
        draws = jax.random.uniform(jax.random.fold_in(jax.random.fold_in(own_key, 6), axis_at), (blocks,), jnp.float32, low / len(shards), top_value / len(shards))
        gain = gain * jnp.repeat(jnp.exp(draws), extent[axis_at] // blocks).reshape((-1,) + (1,) * (len(extent) - 1 - axis_at))
    return gain


def noise(stream_key, extent, scale, most, cuts=(), held_as=jnp.bfloat16):
    factor_of = block_levels(stream_key, extent, cuts, -0.22, 0.18) if cuts else 1.0
    values = jax.random.normal(stream_key, extent, jnp.float32) * scale * factor_of
    return jnp.minimum(jnp.maximum(values, -most), most).astype(held_as)


def setup_inputs(seed: int = 0) -> dict:
    keys = jax.random.split(jax.random.key(seed), 7)
    tokens = draw_tokens(jax.random.fold_in(keys[6], 71), 0)
    phi = draw_phi(jax.random.fold_in(keys[6], 71), 0)
    w_in = noise(keys[2], (EXPERTS, D, FF), D ** -0.5, 0.21875, ((0, 64), (2, 2)))
    w_out = noise(keys[3], (EXPERTS, FF, D), FF ** -0.5, 0.109375, ((0, 64), (1, 2)))
    slot_out = noise(keys[4], (IMAGES, EXPERTS * SLOTS, D), 1.0, 6.0, ((0, 256),))
    grad_out = noise(keys[5], (IMAGES, TOKENS_IMG, D), 1.0, 6.0, ((0, 256),))
    return {"tokens": tokens, "phi": phi, "w_in": w_in, "w_out": w_out, "slot_out": slot_out, "grad_out": grad_out}


def expert_rows(z_rows, g_rows, w_first, w_second):
    pre = jnp.dot(z_rows, w_first, preferred_element_type=jnp.float32)
    act_full, gelu_back = jax.vjp(jax.nn.gelu, pre)
    act = act_full.astype(jnp.bfloat16)
    dact = lax.dot_general(g_rows, w_second, (((1,), (1,)), ((), ())), preferred_element_type=jnp.float32)
    dpre = gelu_back(dact)[0].astype(jnp.bfloat16)
    grad_second = lax.dot_general(act, g_rows, (((0,), (0,)), ((), ())), preferred_element_type=jnp.float32)
    grad_first = lax.dot_general(z_rows, dpre, (((0,), (0,)), ((), ())), preferred_element_type=jnp.float32)
    back = lax.dot_general(dpre, w_first, (((1,), (1,)), ((), ())), preferred_element_type=jnp.float32)
    return (grad_first, grad_second, back)

def reference(tokens, phi, w_in, w_out, slot_out, grad_out):
    f32 = jnp.float32
    logits = jnp.einsum('bmd,ds->bms', tokens.astype(f32), phi.astype(f32))
    dispatch = jax.nn.softmax(logits, axis=1)
    combine = jax.nn.softmax(logits, axis=2)
    dispatch_low = dispatch.astype(jnp.bfloat16)
    combine_low = combine.astype(jnp.bfloat16)
    slot_in = jnp.einsum('bms,bmd->bsd', dispatch_low.astype(f32), tokens.astype(f32)).astype(jnp.bfloat16)
    slot_grad = jnp.einsum('bms,bmd->bsd', combine_low.astype(f32), grad_out.astype(f32)).astype(jnp.bfloat16)
    groups = IMAGES // (N_DP * IMG_DEV)
    per_expert_in = jnp.transpose(slot_in.reshape(IMAGES, EXPERTS, SLOTS, D), (1, 0, 2, 3))
    per_expert_grad = jnp.transpose(slot_grad.reshape(IMAGES, EXPERTS, SLOTS, D), (1, 0, 2, 3))

    def one_expert(items):
        z_all, g_all, w_first, w_second = items
        z_split = z_all.reshape(groups, N_DP, IMG_DEV, SLOTS, D)
        g_split = g_all.reshape(groups, N_DP, IMG_DEV, SLOTS, D)
        total_first = jnp.zeros((D, FF), f32)
        total_second = jnp.zeros((FF, D), f32)
        backs = []
        for index in range(N_DP):
            z_rows = z_split[:, index].reshape(-1, D)
            g_rows = g_split[:, index].reshape(-1, D)
            grad_first, grad_second, back = expert_rows(z_rows, g_rows, w_first, w_second)
            total_first = total_first + grad_first.astype(jnp.bfloat16).astype(f32)
            total_second = total_second + grad_second.astype(jnp.bfloat16).astype(f32)
            backs.append(back.astype(jnp.bfloat16).reshape(groups, 1, IMG_DEV, SLOTS, D))
        back_all = jnp.concatenate(backs, axis=1).reshape(IMAGES, SLOTS, D)
        return (total_first.astype(jnp.bfloat16), total_second.astype(jnp.bfloat16), back_all)
    grad_w_in, grad_w_out, back_experts = lax.map(one_expert, (per_expert_in, per_expert_grad, w_in, w_out))
    slot_in_grad = jnp.transpose(back_experts, (1, 0, 2, 3)).reshape(IMAGES, EXPERTS * SLOTS, D)
    dispatch_grad = jnp.einsum('bmd,bsd->bms', tokens.astype(f32), slot_in_grad.astype(f32))
    combine_grad = jnp.einsum('bmd,bsd->bms', grad_out.astype(f32), slot_out.astype(f32))
    logit_grad = dispatch * (dispatch_grad - lax.optimization_barrier(jnp.sum(dispatch * dispatch_grad, axis=1, keepdims=True)))
    logit_grad = logit_grad + combine * (combine_grad - lax.optimization_barrier(jnp.sum(combine * combine_grad, axis=2, keepdims=True)))
    logit_low = logit_grad.astype(jnp.bfloat16)
    token_part = jnp.einsum('bms,bsd->bmd', dispatch_low.astype(f32), slot_in_grad.astype(f32))
    token_grad = (token_part + jnp.einsum('bms,ds->bmd', logit_low.astype(f32), phi.astype(f32))).astype(jnp.bfloat16)
    phi_grad = jnp.einsum('bmd,bms->ds', tokens.astype(f32), logit_low.astype(f32))
    return (token_grad, phi_grad, grad_w_in, grad_w_out)
```

```python
import jax
import jax.numpy as jnp
import numpy as np
from jax import lax
from jax.sharding import PartitionSpec as P

F32 = jnp.float32
BF16 = jnp.bfloat16
SWAP = [(0, 1), (1, 0)]


def dot(a, b, ca, cb):
    return lax.dot_general(a, b, (((ca,), (cb,)), ((), ())), preferred_element_type=F32)


def one_hot_rows(order):
    order = jnp.asarray(order, jnp.int32)
    return (order[:, None] == jnp.arange(order.shape[0], dtype=jnp.int32)[None, :]).astype(BF16)


def permuted(matrix, rows, transposed=False):
    return dot(matrix, rows, 0 if transposed else 1, 0).astype(BF16)


def expert_back(z, g, w_first, w_second):
    pre = dot(z, w_first, 1, 0)
    act, gelu_back = jax.vjp(jax.nn.gelu, pre)
    dact = dot(g, w_second, 1, 1)
    dpre = gelu_back(dact)[0].astype(BF16)
    return act.astype(BF16), dpre, dot(dpre, w_first, 1, 1)


def summed_over_all(part):
    peers = lax.axis_size("expert")
    rows, lanes = part.shape
    pieces = part.astype(BF16).reshape(peers, rows // peers, lanes)
    got = lax.all_to_all(pieces, "expert", 0, 0, tiled=True)
    mine = jnp.sum(got.astype(F32), axis=0)
    mine = mine + lax.ppermute(mine, "pair", SWAP)
    mine = mine + lax.ppermute(mine, "dp", SWAP)
    spread = jnp.broadcast_to(mine[None], (peers, rows // peers, lanes))
    return lax.all_to_all(spread, "expert", 0, 0, tiled=True).reshape(rows, lanes)


def local(tokens, phi, w_in, w_out, slot_out, grad_out):
    images, _, width = tokens.shape
    n_slots = phi.shape[1]
    experts = lax.axis_size("expert")
    slots = n_slots // experts
    halves = 2
    img = images // halves
    w_first, w_second = w_in[0], w_out[0]
    dp = lax.axis_index("dp")
    half_w = width // 2

    idx = np.arange(2 * img * n_slots).reshape(2, img, experts, slots)
    to_pieces = one_hot_rows(idx.transpose(2, 0, 3, 1).reshape(-1))
    idx = np.arange(2 * img * n_slots).reshape(experts, 2, slots * img)
    by_kind = one_hot_rows(idx.transpose(1, 0, 2).reshape(-1))

    logits = jnp.einsum("bmd,ds->bms", tokens, phi, preferred_element_type=F32)
    dispatch = jax.nn.softmax(logits, axis=1)
    combine = jax.nn.softmax(logits, axis=2)
    dispatch_low = dispatch.astype(BF16)
    combine_low = combine.astype(BF16)
    slot_in = jnp.einsum("bms,bmd->bsd", dispatch_low, tokens, preferred_element_type=F32).astype(BF16)
    slot_grad = jnp.einsum("bms,bmd->bsd", combine_low, grad_out, preferred_element_type=F32).astype(BF16)

    rows = img * n_slots
    own, other = [], []
    for h in range(halves):
        pick = slice(h * img, (h + 1) * img)
        both = jnp.concatenate([slot_in[pick].reshape(rows, width), slot_grad[pick].reshape(rows, width)])
        pieces = permuted(to_pieces, both).reshape(experts, 2 * slots * img, width)
        arrived = lax.all_to_all(pieces, "expert", 0, 0, tiled=True).reshape(2 * rows, width)
        partner = lax.ppermute(arrived, "pair", SWAP)
        own.append(permuted(by_kind, arrived))
        other.append(permuted(by_kind, partner))

    zs, gs, acts, dpres, returned = [], [], [], [], []
    for h in range(halves):
        z = jnp.concatenate([own[h][:rows], other[h][:rows]])
        g = jnp.concatenate([own[h][rows:], other[h][rows:]])
        act, dpre, back = expert_back(z, g, w_first, w_second)
        zs.append(z)
        gs.append(g)
        acts.append(act)
        dpres.append(dpre)
        theirs = lax.ppermute(back[rows:].astype(BF16), "pair", SWAP)
        total = (back[:rows] + theirs.astype(F32)).astype(BF16)
        tall = jnp.concatenate([total[:, :half_w], total[:, half_w:]])
        pieces = permuted(by_kind, tall, True).reshape(experts, 2 * slots * img, half_w)
        got = lax.all_to_all(pieces, "expert", 0, 0, tiled=True).reshape(2 * rows, half_w)
        got = permuted(to_pieces, got, True)
        returned.append(jnp.concatenate([got[:rows], got[rows:]], axis=1).reshape(img, n_slots, width))

    z = jnp.concatenate(zs)
    g = jnp.concatenate(gs)
    act = jnp.concatenate(acts)
    dpre = jnp.concatenate(dpres)

    def columns(array, at):
        return lax.dynamic_slice_in_dim(array, at * half_w, half_w, 1)

    send_first = dot(columns(z, 1 - dp), dpre, 0, 0).astype(BF16)
    send_second = dot(act, columns(g, 1 - dp), 0, 0).astype(BF16)
    got_first = lax.ppermute(send_first, "dp", SWAP)
    got_second = lax.ppermute(send_second, "dp", SWAP)
    keep_first = dot(columns(z, dp), dpre, 0, 0).astype(BF16)
    keep_second = dot(act, columns(g, dp), 0, 0).astype(BF16)
    grad_w_in = (keep_first.astype(F32) + got_first.astype(F32)).astype(BF16)[None]
    grad_w_out = (keep_second.astype(F32) + got_second.astype(F32)).astype(BF16)[None]

    combine_grad = jnp.einsum("bmd,bsd->bms", grad_out, slot_out, preferred_element_type=F32)
    combine_part = combine * (combine_grad - jnp.sum(combine * combine_grad, axis=2, keepdims=True))

    token_grads, phi_part = [], 0.0
    for h in range(halves):
        pick = slice(h * img, (h + 1) * img)
        back = returned[h]
        dispatch_grad = jnp.einsum("bmd,bsd->bms", tokens[pick], back, preferred_element_type=F32)
        mean = jnp.sum(dispatch[pick] * dispatch_grad, axis=1, keepdims=True)
        logit_low = (dispatch[pick] * (dispatch_grad - mean) + combine_part[pick]).astype(BF16)
        token_part = jnp.einsum("bms,bsd->bmd", dispatch_low[pick], back, preferred_element_type=F32)
        token_grads.append(
            (token_part + jnp.einsum("bms,ds->bmd", logit_low, phi, preferred_element_type=F32)).astype(BF16)
        )
        phi_part = phi_part + jnp.einsum("bmd,bms->ds", tokens[pick], logit_low, preferred_element_type=F32)
    return jnp.concatenate(token_grads), summed_over_all(phi_part), grad_w_in, grad_w_out


def solution(mesh):
    in_specs = (
        P(("expert", "pair", "dp"), None, None),
        P(),
        P("expert", None, "pair"),
        P("expert", "pair", None),
        P(("expert", "pair", "dp"), None, None),
        P(("expert", "pair", "dp"), None, None),
    )
    out_specs = (
        P(("expert", "pair", "dp"), None, None),
        P(),
        P("expert", "dp", "pair"),
        P("expert", "pair", "dp"),
    )
    return jax.shard_map(local, mesh=mesh, in_specs=in_specs, out_specs=out_specs, check_vma=False)
```

```python
import functools

import jax
import jax.numpy as jnp
import numpy as np
from jax import lax
from jax.experimental import pallas as pl
from jax.experimental.pallas import tpu as pltpu
from jax.sharding import PartitionSpec as P


F32 = jnp.float32
BF16 = jnp.bfloat16
SWAP = [(0, 1), (1, 0)]
VMEM = 60 * 2**20


def dot(a, b, ca, cb):
    return lax.dot_general(a, b, (((ca,), (cb,)), ((), ())), preferred_element_type=F32)


def split(number, *sizes):
    digits = []
    for size in reversed(sizes):
        digits.append(number & (size - 1))
        number = number >> (size.bit_length() - 1)
    return digits[::-1]


def one_hot(source):
    column = lax.broadcasted_iota(jnp.int32, source.shape, 1)
    return jnp.where(column == source, 1.0, 0.0).astype(BF16)


def to_pieces(experts, slots, img):
    rows = 2 * experts * slots * img
    e, k, j, b = split(lax.broadcasted_iota(jnp.int32, (rows, rows), 0), experts, 2, slots, img)
    return one_hot(((k * img + b) * experts + e) * slots + j)


def by_kind(peers, block):
    rows = 2 * peers * block
    k, e, i = split(lax.broadcasted_iota(jnp.int32, (rows, rows), 0), 2, peers, block)
    return one_hot((e * 2 + k) * block + i)


def expert_kernel(peers, block, w_first, w_second, z, g, act, dpre, back, total):
    step = pl.program_id(0)
    rows = z.shape[0]

    @pl.when(step == 0)
    def _():
        moved = dot(by_kind(peers, rows // peers), block[...], 1, 0).astype(BF16)
        z[...] = moved[:rows]
        g[...] = moved[rows:]
        total[...] = jnp.zeros_like(total)

    x = dot(z[...], w_first[...], 1, 0)
    dact = dot(g[...], w_second[...], 1, 1)
    rate = (2.0 / np.pi) ** 0.5
    square = x * x
    bent = jnp.tanh(rate * (x + 0.044715 * (square * x)))
    share = 0.5 * (1.0 + bent)
    act[...] = (x * share).astype(BF16)
    slope = share + 0.5 * x * (1.0 - bent * bent) * (rate * (1.0 + 3 * 0.044715 * square))
    low = (dact * slope).astype(BF16)
    dpre[...] = low
    total[...] += dot(low, w_first[...], 1, 1)

    @pl.when(step == pl.num_programs(0) - 1)
    def _():
        back[...] = total[...].astype(back.dtype)


def expert_rows(peers, block, w_first, w_second, back_type):
    rows, (width, hidden) = block.shape[0] // 2, w_first.shape
    tile = hidden // 3
    whole = lambda i: (0, 0)
    across = pl.BlockSpec((rows, tile), lambda i: (0, i))
    return pl.pallas_call(
        functools.partial(expert_kernel, peers),
        grid=(3,),
        in_specs=[
            pl.BlockSpec(block.shape, whole),
            pl.BlockSpec((width, tile), lambda i: (0, i)),
            pl.BlockSpec((tile, width), lambda i: (i, 0)),
        ],
        out_specs=[pl.BlockSpec((rows, width), whole)] * 2 + [across] * 2 + [pl.BlockSpec((rows, width), whole)],
        out_shape=[jax.ShapeDtypeStruct((rows, width), BF16)] * 2
        + [jax.ShapeDtypeStruct((rows, hidden), BF16)] * 2
        + [jax.ShapeDtypeStruct((rows, width), back_type)],
        scratch_shapes=[pltpu.VMEM((rows, width), F32)],
        compiler_params=pltpu.CompilerParams(vmem_limit_bytes=VMEM),
        cost_estimate=pl.CostEstimate(
            flops=6 * rows * width * hidden, bytes_accessed=4 * width * hidden, transcendentals=rows * hidden
        ),
    )(block, w_first, w_second)


def sum_kernel(peers, near, far, pieces):
    rows, half = near.shape[0], near.shape[1] // 2
    total = (near[...] + far[...].astype(F32)).astype(BF16)
    tall = jnp.concatenate([total[:, :half], total[:, half:]])
    pieces[...] = dot(by_kind(peers, rows // peers), tall, 0, 0).astype(BF16)


def kernel_call(kernel, arrays, outs, flops, steps=1):
    specs, values = [], []
    for array, first, at in arrays:
        block = array.shape if first is None else (first, *array.shape[1:])
        specs.append(pl.BlockSpec(block, lambda i, at=at, n=array.ndim: (at(i), *(0,) * (n - 1))))
        values.append(array)
    return pl.pallas_call(
        kernel,
        grid=(steps,),
        in_specs=specs,
        out_specs=[
            pl.BlockSpec((o.shape[0] // steps, *o.shape[1:]), lambda i, n=len(o.shape): (i, *(0,) * (n - 1)))
            for o in outs
        ],
        out_shape=outs,
        compiler_params=pltpu.CompilerParams(vmem_limit_bytes=VMEM),
        cost_estimate=pl.CostEstimate(
            flops=flops, bytes_accessed=sum(v.size * v.dtype.itemsize for v in values), transcendentals=0
        ),
    )(*values)


def route_kernel(experts, slots, img, tok, gro, phi, pieces, disp, comb, slots_ref):
    n = phi.shape[1]
    for b in range(img):
        t = tok[b]
        logits = dot(t, phi[...], 1, 0)
        up = jnp.exp(logits - jnp.max(logits, axis=0, keepdims=True))
        d = up / jnp.sum(up, axis=0, keepdims=True)
        across = jnp.exp(logits - jnp.max(logits, axis=1, keepdims=True))
        c = across / jnp.sum(across, axis=1, keepdims=True)
        disp[b] = d
        comb[b] = c
        slots_ref[b * n : (b + 1) * n] = dot(d.astype(BF16), t, 0, 0).astype(BF16)
        slots_ref[(img + b) * n : (img + b + 1) * n] = dot(c.astype(BF16), gro[b], 0, 0).astype(BF16)
    pieces[...] = dot(to_pieces(experts, slots, img), slots_ref[...], 1, 0).astype(BF16)


def slow_kernel(gro, out, comb0, comb1, part):
    c = jnp.where(pl.program_id(0) < pl.num_programs(0) // 2, comb0[0], comb1[0])
    grad = dot(gro[0], out[0], 1, 1)
    part[0] = c * (grad - jnp.sum(c * grad, axis=1, keepdims=True))


def final_kernel(experts, slots, img, tok, disp, part, got, *refs):
    before, (phi_out, low, back) = refs[:-3], refs[-3:]
    n = disp.shape[2]
    half = got.shape[1]
    rows = dot(to_pieces(experts, slots, img), got[...], 0, 0).astype(BF16)
    total = before[0][...] if before else None
    for b in range(img):
        first = rows[b * n : (b + 1) * n]
        second = rows[(img + b) * n : (img + b + 1) * n]
        back[b, :, :half] = first
        back[b, :, half:] = second
        t = tok[b]
        grad = dot(t[:, :half], first, 1, 1) + dot(t[:, half:], second, 1, 1)
        d = disp[b]
        grad = d * (grad - jnp.sum(d * grad, axis=0, keepdims=True)) + part[b]
        grad = grad.astype(BF16)
        low[b] = grad
        term = dot(grad, t, 0, 0)
        total = term if total is None else total + term
    phi_out[...] = total.astype(phi_out.dtype)


def token_kernel(phi, disp0, low0, back0, disp1, low1, back1, out):
    def write(disp, low, back):
        grad = dot(disp[0].astype(BF16), back[0], 1, 0) + dot(low[0], phi[...], 1, 1)
        out[0] = grad.astype(BF16)

    pl.when(pl.program_id(0) < pl.num_programs(0) // 2)(lambda: write(disp0, low0, back0))
    pl.when(pl.program_id(0) >= pl.num_programs(0) // 2)(lambda: write(disp1, low1, back1))


def summed_over_all(part):
    peers = lax.axis_size("expert")
    rows, lanes = part.shape
    pieces = part.reshape(peers, rows // peers, lanes)
    got = lax.all_to_all(pieces, "expert", 0, 0, tiled=True)
    mine = jnp.sum(got.astype(F32), axis=0)
    mine = mine + lax.ppermute(mine, "pair", SWAP)
    mine = mine + lax.ppermute(mine, "dp", SWAP)
    spread = jnp.broadcast_to(mine.astype(BF16)[None], (peers, rows // peers, lanes))
    got = lax.all_to_all(spread, "expert", 0, 0, tiled=True)
    return got.reshape(rows, lanes).astype(F32).T


def body(tokens, phi, w_in, w_out, slot_out, grad_out):
    images, n_tok, width = tokens.shape
    n_slots = phi.shape[1]
    experts = lax.axis_size("expert")
    slots = n_slots // experts
    halves = 2
    img = images // halves
    w_first, w_second = w_in[0], w_out[0]
    dp = lax.axis_index("dp")
    half_w = width // 2
    rows = img * n_slots
    share = jax.ShapeDtypeStruct((img, n_tok, n_slots), F32)
    work = 2 * img * n_tok * n_slots * width
    zero, each = (lambda i: 0), (lambda i: i)
    early, late = (lambda i: jnp.minimum(i, img - 1)), (lambda i: jnp.maximum(i - img, 0))

    disp, comb, arrived, partner = [], [], [], []
    for h in range(halves):
        at_half = lambda i, h=h: h
        pieces, d, c, _ = kernel_call(
            functools.partial(route_kernel, experts, slots, img),
            [(tokens, img, at_half), (grad_out, img, at_half), (phi, None, zero)],
            [jax.ShapeDtypeStruct((2 * rows, width), BF16), share, share, jax.ShapeDtypeStruct((2 * rows, width), BF16)],
            3 * work,
        )
        pieces = pieces.reshape(experts, 2 * slots * img, width)
        disp.append(d)
        comb.append(c)
        arrived.append(lax.all_to_all(pieces, "expert", 0, 0, tiled=True).reshape(2 * rows, width))
        partner.append(lax.ppermute(arrived[h], "pair", SWAP))
    (part,) = kernel_call(
        slow_kernel,
        [(grad_out, 1, each), (slot_out, 1, each), (comb[0], 1, early), (comb[1], 1, late)],
        [jax.ShapeDtypeStruct((images, n_tok, n_slots), F32)],
        2 * work,
        images,
    )

    zs, gs, acts, dpres, returned = [], [], [], [], []
    for h in range(halves):
        for name, block in (("near", arrived[h]), ("far", partner[h])):
            z, g, act, dpre, back = expert_rows(experts, block, w_first, w_second, BF16 if name == "far" else F32)
            zs.append(z)
            gs.append(g)
            acts.append(act)
            dpres.append(dpre)
            if name == "near":
                near = back
        theirs = lax.ppermute(back, "pair", SWAP)
        (pieces,) = kernel_call(
            functools.partial(sum_kernel, experts),
            [(near, None, zero), (theirs, None, zero)],
            [jax.ShapeDtypeStruct((2 * rows, half_w), BF16)],
            work,
        )
        pieces = pieces.reshape(experts, 2 * slots * img, half_w)
        returned.append(lax.all_to_all(pieces, "expert", 0, 0, tiled=True).reshape(2 * rows, half_w))

    z = jnp.concatenate(zs)
    g = jnp.concatenate(gs)
    act = jnp.concatenate(acts)
    dpre = jnp.concatenate(dpres)

    def columns(array, at):
        return lax.dynamic_slice_in_dim(array, at * half_w, half_w, 1)

    send_second = dot(act, columns(g, 1 - dp), 0, 0).astype(BF16)
    send_first = dot(columns(z, 1 - dp), dpre, 0, 0).astype(BF16)
    got_first = lax.ppermute(send_first, "dp", SWAP)
    got_second = lax.ppermute(send_second, "dp", SWAP)
    keep_first = dot(columns(z, dp), dpre, 0, 0).astype(BF16)
    keep_second = dot(act, columns(g, dp), 0, 0).astype(BF16)
    grad_w_in = (keep_first.astype(F32) + got_first.astype(F32)).astype(BF16)[None]
    grad_w_out = (keep_second.astype(F32) + got_second.astype(F32)).astype(BF16)[None]

    phi_part, lows, backs = [], [], []
    for h in range(halves):
        last = h == halves - 1
        at_half = lambda i, h=h: h
        p, low, back = kernel_call(
            functools.partial(final_kernel, experts, slots, img),
            [(tokens, img, at_half), (disp[h], None, zero), (part, img, at_half), (returned[h], None, zero)]
            + [(p, None, zero) for p in phi_part],
            [
                jax.ShapeDtypeStruct((n_slots, width), BF16 if last else F32),
                jax.ShapeDtypeStruct((img, n_tok, n_slots), BF16),
                jax.ShapeDtypeStruct((img, n_slots, width), BF16),
            ],
            2 * work,
        )
        phi_part = [p]
        lows.append(low)
        backs.append(back)
    (token_grad,) = kernel_call(
        token_kernel,
        [(phi, None, zero)]
        + [(x, 1, at) for h, at in ((0, early), (1, late)) for x in (disp[h], lows[h], backs[h])],
        [jax.ShapeDtypeStruct((images, n_tok, width), BF16)],
        4 * work,
        images,
    )
    return token_grad, summed_over_all(phi_part[0]), grad_w_in, grad_w_out


def solution(mesh):
    in_specs = (
        P(("expert", "pair", "dp"), None, None),
        P(),
        P("expert", None, "pair"),
        P("expert", "pair", None),
        P(("expert", "pair", "dp"), None, None),
        P(("expert", "pair", "dp"), None, None),
    )
    out_specs = (
        P(("expert", "pair", "dp"), None, None),
        P(),
        P("expert", "dp", "pair"),
        P("expert", "pair", "dp"),
    )
    return jax.shard_map(body, mesh=mesh, in_specs=in_specs, out_specs=out_specs, check_vma=False)
```
